256 devices in a mesh: mode: 8 (over z), samp: 16 (over y_hi, x, core), pts: 2 (over y_lo).
Axes of the slice: x: 4, y: 4 (y_hi: 2, y_lo: 2; y = y_hi * 2 + y_lo), z: 8, core: 2. Of those that a mesh axis runs over, the one named last changes fastest.
Arguments:
- coefficients: bfloat16 [3072, 12288], P('samp', 'mode'), may hold values from -15 to 15
- panels: bfloat16 [12288, 16384], P(('mode', 'samp'), 'pts'), may hold values from -0.02734375 to 0.02734375
- mean_field: float32 [16384], P('pts'), may hold values from -3 to 3
- load: float32 [16384], P('pts'), may hold values from 0.5 to 2
Outputs:
- standardized: float32 [3072], P('samp')
The draws below stay inside these ranges and needn't reach their ends.
All inputs are finite; a program needn't handle non-finite values.
Results may differ from the reference program's by a relative error of at most 0.0003.
Values may be sent and summed in bfloat16 or wider, within the bound.
No kernel may reach another device: no remote copies, remote signals or barrier semaphores. Data moves between devices by JAX's collectives and lax.ppermute only.
A program may use at most 128 MiB of HBM per device.

```python
import math
import jax
import jax.numpy as jnp
from jax import lax

POINTS = 16384
MODES = 12288
SAMPLES = 3072


def draw_coefficients(key, part):
    first = jax.random.fold_in(key, 11)
    rows = jnp.arange(SAMPLES).astype(jnp.float32)
    scaling = 3.0 ** (rows / (SAMPLES - 1))
    values = jax.random.truncated_normal(first, -4.0, 4.0, (SAMPLES, MODES), jnp.float32)
    return (values * scaling[:, None]).astype(jnp.bfloat16)


def steps_of(stream_key, dims, pieces, least, high):
    factor_of, own = 1.0, jax.random.fold_in(stream_key, 6)
    for axis_at, shards_of in pieces:
        heights = jnp.exp(jax.random.uniform(jax.random.fold_in(own, axis_at), (shards_of,), jnp.float32, least / len(pieces), high / len(pieces)))
        factor_of = factor_of * jnp.repeat(heights, dims[axis_at] // shards_of).reshape([-1 if axis == axis_at else 1 for axis in range(len(dims))])
    return factor_of


def scatter_about(stream_key, shape, deviation, bound, cuts=(), dtype=jnp.bfloat16):
    values = jax.random.normal(stream_key, shape, jnp.float32) * deviation
    if len(cuts) > 0:
        values = steps_of(stream_key, shape, cuts, -0.22, 0.18) * values
    return jnp.clip(values, min=-bound, max=bound).astype(dtype)


def setup_inputs(seed: int = 0) -> dict:
    key_of = jax.random.split(jax.random.key(seed), 5)
    return {
        "coefficients": draw_coefficients(jax.random.fold_in(key_of[4], 71), 0),
        "panels": scatter_about(key_of[1], (MODES, POINTS), (4 * MODES) ** -0.5, 0.02734375, ((0, 128), (1, 2))),
        "mean_field": scatter_about(key_of[2], (POINTS,), 0.5, 3.0, ((0, 2),), jnp.float32),
        "load": jnp.clip(jnp.exp(math.log(2.0) - 1.3862944 * jax.random.uniform(key_of[3], (POINTS,), jnp.float32) ** steps_of(key_of[3], (POINTS,), ((0, 2),), -0.2, 0.2)), 0.5, 2.0),
    }


def reference(coefficients, panels, mean_field, load):
    field = jnp.dot(coefficients, panels, preferred_element_type=jnp.float32) + mean_field[None, :]
    weighted = load[None, :] * jnp.exp(field)
    fine_qoi = lax.optimization_barrier(jnp.sum(weighted, axis=1)) / POINTS
    coarse_qoi = lax.optimization_barrier(jnp.sum(weighted[:, ::2], axis=1)) * (2.0 / POINTS)
    level_diff = fine_qoi - coarse_qoi
    center = jnp.sum(level_diff) / SAMPLES
    spread = jnp.sum((level_diff - center) ** 2) / SAMPLES
    return (level_diff - center) / jnp.sqrt(spread + 1e-06)
```

```python
import jax
import jax.numpy as jnp
from jax import lax
from jax.sharding import Mesh, PartitionSpec as P

POINTS = 16384
SAMPLES = 3072
AXES = ("z", "yh", "x", "c", "yl")
CHUNKS = 2


def shift(array, axis, by):
    n = lax.axis_size(axis)
    return lax.ppermute(array, axis, [(i, (i + by) % n) for i in range(n)])


def over_modes(product, x):
    n = lax.axis_size("z")
    z = lax.axis_index("z")
    rows = product.shape[0] // n
    half = rows // 2

    def block(owner):
        owner = (owner + n) & (n - 1)
        at = ((x - (owner >> 1)) & 3) * (2 * rows) + (owner & 1) * rows
        return lax.dynamic_slice_in_dim(product, at, rows, 0)

    far = block(z + 4)
    down = shift(far[:half], "z", -1)
    up = shift(far[half:], "z", 1)
    for step in (2, 3, 4):
        low, high = block(z - 5 + step), block(z + 5 - step)
        if step == 2:
            low = jnp.concatenate([low[:half] + down, low[half:]], 0)
            high = jnp.concatenate([high[:half], high[half:] + up], 0)
        else:
            low, high = low + down, high + up
        down, up = shift(low, "z", -1), shift(high, "z", 1)
    return block(z) + down + up


def body(coefficients, panels, mean_field, load):
    z, yh, x, c = (lax.axis_index(a) for a in ("z", "yh", "x", "c"))
    samples, modes = coefficients.shape
    rows, points = panels.shape
    parts = coefficients.reshape(samples, 2, 4, 2, rows)
    parts = jnp.where(yh == 1, parts[:, ::-1], parts)
    parts = jnp.where(c == 1, parts[:, :, :, ::-1], parts)
    mine = parts.transpose(0, 1, 3, 2, 4).reshape(samples, modes)
    quarter = points // 4
    width = quarter // CHUNKS
    pieces = panels.reshape(rows, 4, CHUNKS, width)

    def piece(to, k):
        return lax.dynamic_slice(
            pieces, (0, to & 3, k, 0), (rows, 1, 1, width)
        ).reshape(rows, width)

    gathered = [mine] + [shift(mine, "x", r) for r in (1, 2, 3)]
    left = jnp.concatenate(gathered, 0)
    order = (x - jnp.arange(4)) & 3
    sign = jnp.where(jnp.arange(width) % 2 == 1, 1.0, -1.0).astype(jnp.float32)
    total = 0.0
    for k in range(CHUNKS):
        got = [piece(x, k)] + [shift(piece(x + r, k), "x", r) for r in (1, 2, 3)]
        line = jnp.take(jnp.stack(got), order, axis=0, mode="clip").reshape(4 * rows, width)
        other = shift(line, "yh", 1)
        swapped = shift(line, "c", 1)
        other_swapped = shift(other, "c", 1)
        right = jnp.concatenate([line, swapped, other, other_swapped], 0)
        product = jnp.dot(left, right, preferred_element_type=jnp.float32)
        field = over_modes(product, x)
        at = x * quarter + k * width
        mean = lax.dynamic_slice_in_dim(mean_field, at, width, 0)
        weight = lax.dynamic_slice_in_dim(load, at, width, 0) * sign
        total = total + jnp.sum(weight[None, :] * jnp.exp(field + mean[None, :]), axis=1)
    everyone = jnp.broadcast_to(total, (256, *total.shape))
    everyone = lax.all_to_all(everyone, AXES, 0, 0, tiled=True)
    level = jnp.sum(everyone.reshape(8, 2, 4, 2, 2, -1), axis=(2, 4)) / POINTS
    center = jnp.sum(level) / SAMPLES
    spread = jnp.sum((level - center) ** 2) / SAMPLES
    own = lax.dynamic_slice(level, (2 * x, yh, c, 0), (2, 1, 1, level.shape[-1]))
    return (own.reshape(-1) - center) / jnp.sqrt(spread + 1e-06)


def solution(mesh):
    fine = Mesh(mesh.devices.reshape(8, 2, 4, 2, 2), AXES)
    samp = ("yh", "x", "c")
    in_specs = (P(samp, "z"), P(("z",) + samp, "yl"), P("yl"), P("yl"))
    return jax.shard_map(body, mesh=fine, in_specs=in_specs, out_specs=P(samp), check_vma=False)
```

```python
import functools
import jax
import jax.numpy as jnp
from jax import lax
from jax.experimental import pallas as pl
from jax.experimental.pallas import tpu as pltpu
from jax.sharding import Mesh, PartitionSpec as P

POINTS = 16384
SAMPLES = 3072
AXES = ("z", "yh", "x", "c", "yl")
CHUNKS = 2


def shift(array, axis, by):
    n = lax.axis_size(axis)
    return lax.ppermute(array, axis, [(i, (i + by) % n) for i in range(n)])


def product_kernel(own, back, ahead, top, bottom, line, swap, other, both, out, a, b, sem):
    samples, rows = own.shape[0], line.shape[0] // 4
    half = samples // 2

    @pl.when(pl.program_id(0) == 0)
    def _():
        yh, x, c = (lax.axis_index(n) for n in ("yh", "x", "c"))
        copies = []

        def move(source, target):
            copies.append(pltpu.make_async_copy(source, target, sem.at[len(copies)]))

        move(own, a.at[pl.ds(0, samples)])
        move(back, a.at[pl.ds(samples, samples)])
        move(top, a.at[pl.ds(2 * samples, half)])
        move(bottom, a.at[pl.ds(2 * samples + half, half)])
        move(ahead, a.at[pl.ds(3 * samples, samples)])
        for source, y_of, c_of in (
            (line, yh, c), (swap, yh, 1 - c), (other, 1 - yh, c), (both, 1 - yh, 1 - c)
        ):
            for r in range(4):
                at = ((y_of * 4 + lax.rem(x + 4 - r, 4)) * 2 + c_of) * rows
                at = pl.multiple_of(at, 32)
                move(source.at[pl.ds(r * rows, rows)], b.at[pl.ds(at, rows)])
        for copy in copies:
            copy.start()
        for copy in copies:
            copy.wait()

    at = pl.multiple_of(pl.program_id(0) * samples, samples)
    out[...] = jnp.dot(a[pl.ds(at, samples)], b[...], preferred_element_type=jnp.float32)


def product(left, right):
    samples, modes = left[0].shape
    width = right[0].shape[1]
    return pl.pallas_call(
        product_kernel,
        grid=(4,),
        out_shape=jax.ShapeDtypeStruct((4 * samples, width), jnp.float32),
        in_specs=[pl.BlockSpec(memory_space=pl.ANY)] * 9,
        out_specs=pl.BlockSpec((samples, width), lambda i: (i, 0)),
        scratch_shapes=[
            pltpu.VMEM((4 * samples, modes), jnp.bfloat16),
            pltpu.VMEM((modes, width), jnp.bfloat16),
            pltpu.SemaphoreType.DMA((21,)),
        ],
        cost_estimate=pl.CostEstimate(
            flops=8 * samples * modes * width, bytes_accessed=8 << 20, transcendentals=0
        ),
    )(*left, *right)


def over_modes(field, x):
    n = lax.axis_size("z")
    z = lax.axis_index("z")
    rows = field.shape[0] // n
    half = rows // 2

    def block(owner):
        owner = (owner + n) & (n - 1)
        at = ((x - (owner >> 1)) & 3) * (2 * rows) + (owner & 1) * rows
        return lax.dynamic_slice_in_dim(field, at, rows, 0)

    far = block(z + 4)
    low, high = far[:half], far[half:]
    for step in (2, 3, 4):
        down, up = shift(low, "z", -1), shift(high, "z", 1)
        low, high = block(z - 5 + step), block(z + 5 - step)
        if step == 2:
            low = jnp.concatenate([low[:half] + down, low[half:]], 0)
            high = jnp.concatenate([high[:half], high[half:] + up], 0)
        else:
            low, high = low + down, high + up
        yield low, high
    down, up = shift(low, "z", -1), shift(high, "z", 1)
    yield block(z) + down + up


def body(coefficients, panels, mean_field, load):
    yh, x, c = (lax.axis_index(a) for a in ("yh", "x", "c"))
    samples, modes = coefficients.shape
    rows, points = panels.shape
    half = samples // 2
    quarter = points // 4
    width = quarter // CHUNKS

    def pieces_of(k):
        def piece(to):
            at = (to & 3) * quarter + k * width
            return lax.dynamic_slice(panels, (0, at), (rows, width))

        return [piece(x + r) for r in range(4)]

    def spread(pieces):
        return pieces[:1] + [shift(pieces[r], "x", r) for r in (1, 2, 3)]

    first = spread(pieces_of(0))
    second = pieces_of(1)
    coefficients, *_ = lax.optimization_barrier((coefficients, first[1], first[3]))
    back, ahead = shift(coefficients, "x", 1), shift(coefficients, "x", -1)
    top, bottom = shift(back[:half], "x", 1), shift(ahead[half:], "x", -1)
    left = (coefficients, back, ahead, top, bottom)

    sign = jnp.where(jnp.arange(width) % 2 == 1, 1.0, -1.0).astype(jnp.float32)

    def line_and_other(pieces):
        line = jnp.concatenate(pieces, 0)
        return line, shift(line, "yh", 1)

    def factor(line, other):
        return line, shift(line, "c", 1), other, shift(other, "c", 1)

    def after(value, *others):
        return lax.optimization_barrier((value, *others))[0]

    def contribution(field, k):
        at = x * quarter + k * width
        mean = lax.dynamic_slice_in_dim(mean_field, at, width, 0)
        weight = lax.dynamic_slice_in_dim(load, at, width, 0) * sign
        return jnp.sum(weight[None, :] * jnp.exp(field + mean[None, :]), axis=1)

    matrix = product(left, factor(*line_and_other(first)))
    chain = over_modes(matrix, x)
    second, *_ = lax.optimization_barrier((second, top, bottom))
    second = spread(second)
    second[0] = after(second[0], matrix)
    line, other = line_and_other(second)
    state = next(chain)
    line, swap, other, both = factor(line, after(other, state))
    state = next(chain)
    chain_too = over_modes(product(left, (line, swap, other, after(both, state))), x)
    fields = [list(c)[-1] for c in (chain, chain_too)]
    total = contribution(fields[0], 0) + contribution(fields[1], 1)
    everyone = jnp.broadcast_to(total, (256, *total.shape))
    everyone = lax.all_to_all(everyone, AXES, 0, 0, tiled=True)
    level = jnp.sum(everyone.reshape(8, 2, 4, 2, 2, -1), axis=(2, 4)) / POINTS
    center = jnp.sum(level) / SAMPLES
    spread = jnp.sum((level - center) ** 2) / SAMPLES
    own = lax.dynamic_slice(level, (2 * x, yh, c, 0), (2, 1, 1, level.shape[-1]))
    return (own.reshape(-1) - center) / jnp.sqrt(spread + 1e-06)


def solution(mesh):
    fine = Mesh(mesh.devices.reshape(8, 2, 4, 2, 2), AXES)
    samp = ("yh", "x", "c")
    in_specs = (P(samp, "z"), P(("z",) + samp, "yl"), P("yl"), P("yl"))
    return jax.shard_map(body, mesh=fine, in_specs=in_specs, out_specs=P(samp), check_vma=False)
```

```python
import jax
import jax.numpy as jnp
from jax import lax
from jax.experimental import pallas as pl
from jax.experimental.pallas import tpu as pltpu
from jax.sharding import Mesh, PartitionSpec as P

POINTS = 16384
SAMPLES = 3072
AXES = ("z", "yh", "x", "c", "yl")


def shift(array, axis, by):
    n = lax.axis_size(axis)
    return lax.ppermute(array, axis, [(i, (i + by) % n) for i in range(n)])


def split_kernel(panels, *refs):
    pieces, sem = refs[:4], refs[4]
    width = pieces[0].shape[1]
    x = lax.axis_index("x")
    copies = []
    for r in range(4):
        at = pl.multiple_of(lax.rem(x + r, 4) * width, width)
        copies.append(pltpu.make_async_copy(panels.at[:, pl.ds(at, width)], pieces[r], sem.at[r]))
    for copy in copies:
        copy.start()
    for copy in copies:
        copy.wait()


def split(panels):
    rows, points = panels.shape
    return pl.pallas_call(
        split_kernel,
        out_shape=[jax.ShapeDtypeStruct((rows, points // 4), panels.dtype)] * 4,
        in_specs=[pl.BlockSpec(memory_space=pl.ANY)],
        out_specs=[pl.BlockSpec(memory_space=pl.ANY)] * 4,
        scratch_shapes=[pltpu.SemaphoreType.DMA((4,))],
    )(panels)


def product_kernel(own, back, ahead, top, bottom, *refs):
    pieces, (*outs, a, b, sem) = refs[:-5], refs[-5:]
    samples, rows = own.shape[0], pieces[0].shape[0]
    half = samples // 2
    j, i = pl.program_id(0), pl.program_id(1)

    @pl.when((j == 0) & (i == 0))
    def _():
        yh, x, c = (lax.axis_index(n) for n in ("yh", "x", "c"))
        copies = []

        def move(source, target):
            copies.append(pltpu.make_async_copy(source, target, sem.at[len(copies)]))

        move(own, a.at[pl.ds(0, samples)])
        move(back, a.at[pl.ds(samples, samples)])
        move(top, a.at[pl.ds(2 * samples, half)])
        move(bottom, a.at[pl.ds(2 * samples + half, half)])
        move(ahead, a.at[pl.ds(3 * samples, samples)])
        for n, source in enumerate(pieces):
            y_of = yh if n < 8 else 1 - yh
            c_of = c if n % 8 < 4 else 1 - c
            at = ((y_of * 4 + lax.rem(x + 4 - n % 4, 4)) * 2 + c_of) * rows
            move(source, b.at[pl.ds(pl.multiple_of(at, 32), rows)])
        for copy in copies:
            copy.start()
        for copy in copies:
            copy.wait()

    row = pl.multiple_of(i * samples, samples)
    for k, out in enumerate(outs):
        width = out.shape[1]

        @pl.when(j == k)
        def _():
            out[...] = jnp.dot(
                a[pl.ds(row, samples)],
                b[:, k * width : (k + 1) * width],
                preferred_element_type=jnp.float32,
            )


def product(left, right):
    samples, modes = left[0].shape
    width = right[0].shape[1]
    return pl.pallas_call(
        product_kernel,
        grid=(2, 4),
        out_shape=[jax.ShapeDtypeStruct((4 * samples, width // 2), jnp.float32)] * 2,
        in_specs=[pl.BlockSpec(memory_space=pl.ANY)] * 21,
        out_specs=[
            pl.BlockSpec((samples, width // 2), lambda j, i: (i * (1 - j) + 3 * j, 0)),
            pl.BlockSpec((samples, width // 2), lambda j, i: (i * j, 0)),
        ],
        scratch_shapes=[
            pltpu.VMEM((4 * samples, modes), jnp.bfloat16),
            pltpu.VMEM((modes, width), jnp.bfloat16),
            pltpu.SemaphoreType.DMA((21,)),
        ],
        cost_estimate=pl.CostEstimate(
            flops=8 * samples * modes * width, bytes_accessed=16 << 20, transcendentals=0
        ),
    )(*left, *right)


def over_modes(fields, x):
    n = lax.axis_size("z")
    z = lax.axis_index("z")
    rows = fields[0].shape[0] // n

    def block(owner, k):
        owner = (owner + n) & (n - 1)
        at = ((x - (owner >> 1)) & 3) * (2 * rows) + (owner & 1) * rows
        return lax.dynamic_slice_in_dim(fields[k], at, rows, 0)

    far = (-1, 1)
    long = [block(z - 4 * far[k], k) for k in (0, 1)]
    short = [block(z - 3 * far[k], k) for k in (0, 1)]
    for hop in (1, 2, 3):
        for k in (0, 1):
            long[k] = shift(long[k], "z", far[k])
            short[k] = shift(short[k], "z", -far[k])
            long[k] = long[k] + block(z + (4 - hop) * far[k], k)
            if hop < 3:
                short[k] = short[k] + block(z - (3 - hop) * far[k], k)
    return [shift(long[k], "z", far[k]) + short[k] + block(z, k) for k in (0, 1)]


def body(coefficients, panels, mean_field, load):
    yh, x, c = (lax.axis_index(a) for a in ("yh", "x", "c"))
    samples = coefficients.shape[0]
    half = samples // 2
    quarter = panels.shape[1] // 4

    pieces = split(panels)
    line = [pieces[0]] + [shift(pieces[r], "x", r) for r in (1, 2, 3)]
    other = [shift(piece, "yh", 1) for piece in line]
    mine, *_ = lax.optimization_barrier((coefficients, line[1], line[3]))
    back, ahead = shift(mine, "x", 1), shift(mine, "x", -1)
    top, bottom = shift(back[:half], "x", 1), shift(ahead[half:], "x", -1)
    swap = [shift(piece, "c", 1) for piece in line]
    both = [shift(piece, "c", 1) for piece in other]
    fields = product((mine, back, ahead, top, bottom), (*line, *swap, *other, *both))

    width = quarter // 2
    sign = jnp.where(jnp.arange(width) % 2 == 1, 1.0, -1.0).astype(jnp.float32)
    total = 0.0
    for k, part in enumerate(over_modes(fields, x)):
        at = x * quarter + k * width
        mean = lax.dynamic_slice_in_dim(mean_field, at, width, 0)
        weight = lax.dynamic_slice_in_dim(load, at, width, 0) * sign
        total = total + jnp.sum(weight[None, :] * jnp.exp(part + mean[None, :]), axis=1)
    everyone = jnp.broadcast_to(total, (256, *total.shape))
    everyone = lax.all_to_all(everyone, AXES, 0, 0, tiled=True)
    level = jnp.sum(everyone.reshape(8, 2, 4, 2, 2, -1), axis=(2, 4)) / POINTS
    center = jnp.sum(level) / SAMPLES
    spread = jnp.sum((level - center) ** 2) / SAMPLES
    own = lax.dynamic_slice(level, (2 * x, yh, c, 0), (2, 1, 1, level.shape[-1]))
    return (own.reshape(-1) - center) / jnp.sqrt(spread + 1e-06)


def solution(mesh):
    fine = Mesh(mesh.devices.reshape(8, 2, 4, 2, 2), AXES)
    samp = ("yh", "x", "c")
    in_specs = (P(samp, "z"), P(("z",) + samp, "yl"), P("yl"), P("yl"))
    return jax.shard_map(body, mesh=fine, in_specs=in_specs, out_specs=P(samp), check_vma=False)
```

```python
import functools
import jax
import jax.numpy as jnp
from jax import lax
from jax.experimental import pallas as pl
from jax.experimental.pallas import tpu as pltpu
from jax.sharding import Mesh, PartitionSpec as P

POINTS = 16384
SAMPLES = 3072
AXES = ("z", "yh", "x", "c", "yl")


def shift(array, axis, by):
    n = lax.axis_size(axis)
    return lax.ppermute(array, axis, [(i, (i + by) % n) for i in range(n)])


def split_kernel(panels, *refs):
    pieces, sem = refs[:4], refs[4]
    width = pieces[0].shape[1]
    x = lax.axis_index("x")
    copies = []
    for r in range(4):
        at = pl.multiple_of(lax.rem(x + r, 4) * width, width)
        copies.append(pltpu.make_async_copy(panels.at[:, pl.ds(at, width)], pieces[r], sem.at[r]))
    for copy in copies:
        copy.start()
    for copy in copies:
        copy.wait()


def split(panels):
    rows, points = panels.shape
    return pl.pallas_call(
        split_kernel,
        out_shape=[jax.ShapeDtypeStruct((rows, points // 4), panels.dtype)] * 4,
        in_specs=[pl.BlockSpec(memory_space=pl.ANY)],
        out_specs=[pl.BlockSpec(memory_space=pltpu.VMEM)] * 4,
        scratch_shapes=[pltpu.SemaphoreType.DMA((4,))],
    )(panels)


def product_kernel(own, back, ahead, top, bottom, *refs):
    pieces, (*outs, a, b, sem) = refs[:-5], refs[-5:]
    samples, rows = own.shape[0], pieces[0].shape[0]
    half = samples // 2
    width = outs[0].shape[1]
    steps = b.shape[1] // width // 2
    j = pl.program_id(0)
    yh, x, c = (lax.axis_index(n) for n in ("yh", "x", "c"))
    columns = [pl.ds(k * steps * width, steps * width) for k in range(2)]
    copies = [[], []]

    def move(k, source, target):
        number = len(copies[0]) + len(copies[1])
        copies[k].append(pltpu.make_async_copy(source, target, sem.at[number]))

    move(0, own, a.at[pl.ds(0, samples)])
    move(0, back, a.at[pl.ds(samples, samples)])
    move(0, top, a.at[pl.ds(2 * samples, half)])
    move(0, bottom, a.at[pl.ds(2 * samples + half, half)])
    move(0, ahead, a.at[pl.ds(3 * samples, samples)])
    for k in range(2):
        for n, source in enumerate(pieces):
            y_of = yh if n < 8 else 1 - yh
            c_of = c if n % 8 < 4 else 1 - c
            at = ((y_of * 4 + lax.rem(x + 4 - n % 4, 4)) * 2 + c_of) * rows
            at = pl.multiple_of(at, 32)
            move(k, source.at[:, columns[k]], b.at[pl.ds(at, rows), columns[k]])

    @pl.when(j == 0)
    def _():
        for copy in copies[0] + copies[1]:
            copy.start()

    for k, out in enumerate(outs):
        @pl.when(j == k * steps)
        def _():
            for copy in copies[k]:
                copy.wait()

        @pl.when((j >= k * steps) & (j < (k + 1) * steps))
        def _():
            at = pl.multiple_of(j * width, width)
            out[...] = jnp.dot(a[...], b[:, pl.ds(at, width)], preferred_element_type=jnp.float32)


def product(left, right):
    samples, modes = left[0].shape
    width = right[0].shape[1]
    block, steps = 256, width // 512
    return pl.pallas_call(
        product_kernel,
        grid=(2 * steps,),
        out_shape=[jax.ShapeDtypeStruct((4 * samples, width // 2), jnp.float32)] * 2,
        in_specs=[pl.BlockSpec(memory_space=pl.ANY)] * 21,
        out_specs=[
            pl.BlockSpec((4 * samples, block), lambda j: (0, jnp.minimum(j, steps - 1))),
            pl.BlockSpec((4 * samples, block), lambda j: (0, jnp.maximum(j - steps, 0))),
        ],
        scratch_shapes=[
            pltpu.VMEM((4 * samples, modes), jnp.bfloat16),
            pltpu.VMEM((modes, width), jnp.bfloat16),
            pltpu.SemaphoreType.DMA((37,)),
        ],
        cost_estimate=pl.CostEstimate(
            flops=8 * samples * modes * width, bytes_accessed=16 << 20, transcendentals=0
        ),
    )(*left, *right)


SPAN = 250.0
TAIL = 16
ANY = pl.BlockSpec(memory_space=pl.ANY)
VMEM = pl.BlockSpec(memory_space=pltpu.VMEM)


def encode(out, values):
    rows = values[0].shape[0]
    largest = functools.reduce(jnp.maximum, [jnp.abs(v) for v in values])
    scale = jnp.maximum(jnp.max(largest, axis=0, keepdims=True), 1e-30) * 1.01
    scale = scale.astype(jnp.bfloat16)
    factor = SPAN / scale.astype(jnp.float32)
    for q, v in enumerate(values):
        code = jnp.exp2(jnp.abs(v) * factor - SPAN / 2)
        out[q * rows : (q + 1) * rows, :] = jnp.where(v < 0, -code, code).astype(jnp.bfloat16)
    out[len(values) * rows :, :] = jnp.broadcast_to(scale, (TAIL, 128))


def decode(message, rows, count):
    scale = message[count * rows :, :].astype(jnp.float32)[:1] / SPAN
    values = []
    for q in range(count):
        code = message[q * rows : (q + 1) * rows, :].astype(jnp.float32)
        size = (jnp.log2(jnp.abs(code)) + SPAN / 2) * scale
        values.append(jnp.where(code < 0, -size, size))
    return values


def row_of(offset, rows):
    z, x = lax.axis_index("z"), lax.axis_index("x")
    owner = (z + offset + 8) & 7
    return pl.multiple_of(((x - (owner >> 1)) & 3) * (2 * rows) + (owner & 1) * rows, rows)


def columns_of(block):
    return [block[:, q * 128 : (q + 1) * 128] for q in range(block.shape[1] // 128)]


def hop_kernel(offsets, first, *refs):
    n = len(offsets)
    messages, refs = ([], refs) if first else (refs[:n], refs[n:])
    matrix, outs, (blocks, sem) = refs[0], refs[1 : 1 + n], refs[1 + n :]
    rows, count = blocks.shape[1], blocks.shape[2] // 128
    loads = []
    for m, offset in enumerate(offsets):
        source = matrix.at[pl.ds(row_of(offset, rows), rows)]
        loads.append(pltpu.make_async_copy(source, blocks.at[m], sem.at[m]))
    for load in loads:
        load.start()
    for m in range(n):
        values = [] if first else decode(messages[m], rows, count)
        loads[m].wait()
        own = columns_of(blocks[m])
        encode(outs[m], own if first else [u + v for u, v in zip(values, own)])


def hop(messages, matrix, offsets):
    n, (rows, width) = len(offsets), (matrix.shape[0] // 8, matrix.shape[1])
    shape = (rows * width // 128 + TAIL, 128)
    return pl.pallas_call(
        functools.partial(hop_kernel, offsets, not messages),
        out_shape=[jax.ShapeDtypeStruct(shape, jnp.bfloat16)] * n,
        in_specs=[VMEM] * len(messages) + [ANY],
        out_specs=[VMEM] * n,
        scratch_shapes=[
            pltpu.VMEM((n, rows, width), jnp.float32),
            pltpu.SemaphoreType.DMA((n,)),
        ],
        cost_estimate=pl.CostEstimate(
            flops=1 << 30, bytes_accessed=2 << 20, transcendentals=n << 18
        ),
    )(*messages, matrix)


def finish_kernel(messages, matrix, matrix_too, mean, load, out, blocks, sem):
    rows, count = blocks.shape[1], blocks.shape[2] // 128
    loads = []
    for k, source in enumerate((matrix, matrix_too)):
        source = source.at[pl.ds(row_of(0, rows), rows)]
        loads.append(pltpu.make_async_copy(source, blocks.at[k], sem.at[k]))
    for copy in loads:
        copy.start()
    for copy in loads:
        copy.wait()
    x = lax.axis_index("x")
    odd = lax.rem(lax.broadcasted_iota(jnp.int32, (1, 128), 1), 2)
    sign = jnp.where(odd == 1, 1.0, -1.0)
    total = jnp.zeros((rows, 128), jnp.float32)
    for k in range(2):
        parts = [columns_of(blocks[k])]
        parts += [decode(messages[2 * k + m], rows, count) for m in range(2)]
        for q in range(count):
            at = pl.ds((x * 2 + k) * count + q, 1)
            field = parts[0][q] + parts[1][q] + parts[2][q] + mean[at, :]
            total = total + (load[at, :] * sign) * jnp.exp(field)
    out[...] = total


def finish(messages, matrices, mean, load):
    rows, width = matrices[0].shape[0] // 8, matrices[0].shape[1]

    def kernel(*refs):
        finish_kernel(refs[:4], *refs[4:])

    return pl.pallas_call(
        kernel,
        out_shape=jax.ShapeDtypeStruct((rows, 128), jnp.float32),
        in_specs=[VMEM] * 4 + [ANY] * 2 + [VMEM] * 2,
        out_specs=VMEM,
        scratch_shapes=[
            pltpu.VMEM((2, rows, width), jnp.float32),
            pltpu.SemaphoreType.DMA((2,)),
        ],
    )(*messages, *matrices, mean.reshape(-1, 128), load.reshape(-1, 128))


def over_modes(matrices):
    far = (-1, 1)
    state = [hop([], m, (4 * f, -3 * f)) for m, f in zip(matrices, far)]
    arrived = [None, None]
    for step in (3, 2, 1):
        for k, f in enumerate(far):
            long = shift(state[k][0], "z", f)
            short = shift(state[k][1], "z", -f) if state[k][1:] else arrived[k]
            if step > 1:
                state[k] = hop([long, short], matrices[k], (step * f, -(step - 1) * f))
            else:
                arrived[k] = short
                state[k] = hop([long], matrices[k], (f,))
    return [m for k, f in enumerate(far) for m in (shift(state[k][0], "z", f), arrived[k])]


def body(coefficients, panels, mean_field, load):
    yh, x, c = (lax.axis_index(a) for a in ("yh", "x", "c"))
    samples = coefficients.shape[0]
    half = samples // 2
    quarter = panels.shape[1] // 4

    pieces = split(panels)
    line = [pieces[0]] + [shift(pieces[r], "x", r) for r in (1, 2, 3)]
    other = [shift(piece, "yh", 1) for piece in line]
    mine, *_ = lax.optimization_barrier((coefficients, line[1], line[3], other[0]))
    back, ahead = shift(mine, "x", 1), shift(mine, "x", -1)
    top, bottom = shift(back[:half], "x", 1), shift(ahead[half:], "x", -1)
    swap = [shift(piece, "c", 1) for piece in line]
    late, *_ = lax.optimization_barrier((other[1:], top, bottom))
    both = [shift(piece, "c", 1) for piece in (other[0], *late)]
    matrices = product((mine, back, ahead, top, bottom), (*line, *swap, *other, *both))
    total = jnp.sum(finish(over_modes(matrices), matrices, mean_field, load), axis=1)
    everyone = jnp.broadcast_to(total, (256, *total.shape))
    everyone = lax.all_to_all(everyone, AXES, 0, 0, tiled=True)
    level = jnp.sum(everyone.reshape(8, 2, 4, 2, 2, -1), axis=(2, 4)) / POINTS
    center = jnp.sum(level) / SAMPLES
    spread = jnp.sum((level - center) ** 2) / SAMPLES
    own = lax.dynamic_slice(level, (2 * x, yh, c, 0), (2, 1, 1, level.shape[-1]))
    return (own.reshape(-1) - center) / jnp.sqrt(spread + 1e-06)


def solution(mesh):
    fine = Mesh(mesh.devices.reshape(8, 2, 4, 2, 2), AXES)
    samp = ("yh", "x", "c")
    in_specs = (P(samp, "z"), P(("z",) + samp, "yl"), P("yl"), P("yl"))
    return jax.shard_map(body, mesh=fine, in_specs=in_specs, out_specs=P(samp), check_vma=False)
```

```python
import functools
import jax
import jax.numpy as jnp
from jax import lax
from jax.experimental import pallas as pl
from jax.experimental.pallas import tpu as pltpu
from jax.sharding import Mesh, PartitionSpec as P

POINTS = 16384
SAMPLES = 3072
AXES = ("z", "yh", "x", "c", "yl")


def shift(array, axis, by):
    n = lax.axis_size(axis)
    return lax.ppermute(array, axis, [(i, (i + by) % n) for i in range(n)])


def split_kernel(panels, *refs):
    pieces, sem = refs[:4], refs[4]
    width = pieces[0].shape[1]
    x = lax.axis_index("x")
    copies = []
    for r in range(4):
        at = pl.multiple_of(lax.rem(x + r, 4) * width, width)
        copies.append(pltpu.make_async_copy(panels.at[:, pl.ds(at, width)], pieces[r], sem.at[r]))
    for copy in copies:
        copy.start()
    for copy in copies:
        copy.wait()


def split(panels):
    rows, points = panels.shape
    return pl.pallas_call(
        split_kernel,
        out_shape=[pltpu.VMEM((rows, points // 4), panels.dtype)] * 4,
        in_specs=[pl.BlockSpec(memory_space=pl.ANY)],
        out_specs=[pl.BlockSpec(memory_space=pltpu.VMEM)] * 4,
        scratch_shapes=[pltpu.SemaphoreType.DMA((4,))],
        compiler_params=pltpu.CompilerParams(vmem_limit_bytes=4 << 20),
    )(pltpu.with_memory_space_constraint(panels, pltpu.HBM))


ANY = pl.BlockSpec(memory_space=pl.ANY)
VMEM = pl.BlockSpec(memory_space=pltpu.VMEM)


def on_chip(arrays):
    return [pltpu.with_memory_space_constraint(a, pltpu.VMEM) for a in arrays]


def product_kernel(own, back, ahead, top, bottom, *refs):
    pieces, (*outs, a, b, sem) = refs[:-5], refs[-5:]
    samples, rows = own.shape[0], pieces[0].shape[0]
    half = samples // 2
    yh, x, c = (lax.axis_index(n) for n in ("yh", "x", "c"))
    copies = []

    def move(source, target):
        copies.append(pltpu.make_async_copy(source, target, sem.at[len(copies)]))

    move(own, a.at[pl.ds(0, samples)])
    move(back, a.at[pl.ds(samples, samples)])
    move(top, a.at[pl.ds(2 * samples, half)])
    move(bottom, a.at[pl.ds(2 * samples + half, half)])
    move(ahead, a.at[pl.ds(3 * samples, samples)])
    for n, source in enumerate(pieces):
        y_of = yh if n < 8 else 1 - yh
        c_of = c if n % 8 < 4 else 1 - c
        at = ((y_of * 4 + lax.rem(x + 4 - n % 4, 4)) * 2 + c_of) * rows
        move(source, b.at[pl.ds(pl.multiple_of(at, 32), rows)])
    for copy in copies:
        copy.start()
    for copy in copies:
        copy.wait()
    width = 256
    for k, out in enumerate(outs):
        for at in range(0, out.shape[1], width):
            first = k * out.shape[1] + at
            out[:, at : at + width] = jnp.dot(
                a[...], b[:, first : first + width], preferred_element_type=jnp.float32
            )


def product(left, right):
    samples, modes = left[0].shape
    width = right[0].shape[1]
    return pl.pallas_call(
        product_kernel,
        out_shape=[pltpu.VMEM((4 * samples, width // 2), jnp.float32)] * 2,
        in_specs=[ANY] + [VMEM] * 20,
        compiler_params=pltpu.CompilerParams(vmem_limit_bytes=24 << 20),
        out_specs=[VMEM] * 2,
        scratch_shapes=[
            pltpu.VMEM((4 * samples, modes), jnp.bfloat16),
            pltpu.VMEM((modes, width), jnp.bfloat16),
            pltpu.SemaphoreType.DMA((21,)),
        ],
        cost_estimate=pl.CostEstimate(
            flops=8 * samples * modes * width, bytes_accessed=16 << 20, transcendentals=0
        ),
    )(pltpu.with_memory_space_constraint(left[0], pltpu.HBM), *on_chip((*left[1:], *right)))


SPAN = 250.0
TAIL = 16


def encode(out, values):
    rows = values[0].shape[0]
    largest = functools.reduce(jnp.maximum, [jnp.abs(v) for v in values])
    scale = jnp.maximum(jnp.max(largest, axis=0, keepdims=True), 1e-30) * 1.01
    scale = scale.astype(jnp.bfloat16)
    factor = SPAN / scale.astype(jnp.float32)
    for q, v in enumerate(values):
        code = jnp.exp2(jnp.abs(v) * factor - SPAN / 2)
        out[q * rows : (q + 1) * rows, :] = jnp.where(v < 0, -code, code).astype(jnp.bfloat16)
    out[len(values) * rows :, :] = jnp.broadcast_to(scale, (TAIL, 128))


def decode(message, rows, count):
    scale = message[count * rows :, :].astype(jnp.float32)[:1] / SPAN
    values = []
    for q in range(count):
        code = message[q * rows : (q + 1) * rows, :].astype(jnp.float32)
        size = (jnp.log2(jnp.abs(code)) + SPAN / 2) * scale
        values.append(jnp.where(code < 0, -size, size))
    return values


def row_of(offset, rows):
    z, x = lax.axis_index("z"), lax.axis_index("x")
    owner = (z + offset + 8) & 7
    return pl.multiple_of(((x - (owner >> 1)) & 3) * (2 * rows) + (owner & 1) * rows, rows)


def columns_of(block):
    return [block[:, q * 128 : (q + 1) * 128] for q in range(block.shape[1] // 128)]


def hop_kernel(offsets, first, *refs):
    n = len(offsets)
    messages, refs = ([], refs) if first else (refs[:n], refs[n:])
    matrix, outs = refs[0], refs[1:]
    rows, count = matrix.shape[0] // 8, matrix.shape[1] // 128
    for m, offset in enumerate(offsets):
        own = columns_of(matrix[pl.ds(row_of(offset, rows), rows), :])
        if not first:
            own = [u + v for u, v in zip(own, decode(messages[m], rows, count))]
        encode(outs[m], own)


def hop(messages, matrix, offsets):
    n, (rows, width) = len(offsets), (matrix.shape[0] // 8, matrix.shape[1])
    shape = (rows * width // 128 + TAIL, 128)
    return pl.pallas_call(
        functools.partial(hop_kernel, offsets, not messages),
        out_shape=[pltpu.VMEM(shape, jnp.bfloat16)] * n,
        in_specs=[VMEM] * (len(messages) + 1),
        compiler_params=pltpu.CompilerParams(vmem_limit_bytes=8 << 20),
        out_specs=[VMEM] * n,
        cost_estimate=pl.CostEstimate(
            flops=1 << 30, bytes_accessed=2 << 20, transcendentals=n << 18
        ),
    )(*on_chip((*messages, matrix)))


def finish_kernel(*refs):
    messages, matrices, (mean, load, out) = refs[:4], refs[4:6], refs[6:]
    rows, count = matrices[0].shape[0] // 8, matrices[0].shape[1] // 128
    x = lax.axis_index("x")
    odd = lax.rem(lax.broadcasted_iota(jnp.int32, (1, 128), 1), 2)
    sign = jnp.where(odd == 1, 1.0, -1.0)
    total = jnp.zeros((rows, 128), jnp.float32)
    for k in range(2):
        parts = [columns_of(matrices[k][pl.ds(row_of(0, rows), rows), :])]
        parts += [decode(messages[2 * k + m], rows, count) for m in range(2)]
        for q in range(count):
            at = pl.ds((x * 2 + k) * count + q, 1)
            field = parts[0][q] + parts[1][q] + parts[2][q] + mean[at, :]
            total = total + (load[at, :] * sign) * jnp.exp(field)
    out[...] = total


def finish(messages, matrices, mean, load):
    rows = matrices[0].shape[0] // 8
    return pl.pallas_call(
        finish_kernel,
        out_shape=jax.ShapeDtypeStruct((rows, 128), jnp.float32),
        in_specs=[VMEM] * 8,
        compiler_params=pltpu.CompilerParams(vmem_limit_bytes=8 << 20),
        out_specs=VMEM,
    )(*on_chip((*messages, *matrices)), mean.reshape(-1, 128), load.reshape(-1, 128))


def over_modes(matrices):
    far = (-1, 1)
    state = [hop([], m, (4 * f, -3 * f)) for m, f in zip(matrices, far)]
    arrived = [None, None]
    for step in (3, 2, 1):
        for k, f in enumerate(far):
            long = shift(state[k][0], "z", f)
            short = shift(state[k][1], "z", -f) if state[k][1:] else arrived[k]
            if step > 1:
                state[k] = hop([long, short], matrices[k], (step * f, -(step - 1) * f))
            else:
                arrived[k] = short
                state[k] = hop([long], matrices[k], (f,))
    return [m for k, f in enumerate(far) for m in (shift(state[k][0], "z", f), arrived[k])]


def level_correction(coefficients, panels, mean_field, load):
    yh, x, c = (lax.axis_index(a) for a in ("yh", "x", "c"))
    samples = coefficients.shape[0]
    half = samples // 2

    pieces = split(panels)
    line = [pieces[0], *(shift(pieces[r], "x", r) for r in (1, 2, 3))]
    line[2] = shift(pieces[2], "x", 2)
    other = [shift(piece, "yh", 1) for piece in line]
    mine, *_ = lax.optimization_barrier((coefficients, line[1], line[3], other[0]))
    back = shift(mine, "x", 1)
    ahead = shift(mine, "x", -1)
    top, bottom = shift(back[:half], "x", 1), shift(ahead[half:], "x", -1)
    swap = [shift(piece, "c", 1) for piece in line]
    late, *_ = lax.optimization_barrier((other[1:], top, bottom))
    both = [shift(piece, "c", 1) for piece in (other[0], *late)]
    matrices = product((mine, back, ahead, top, bottom), (*line, *swap, *other, *both))
    total = jnp.sum(finish(over_modes(matrices), matrices, mean_field, load), axis=1)
    everyone = jnp.broadcast_to(total, (256, *total.shape))
    everyone = lax.all_to_all(everyone, AXES, 0, 0, tiled=True)
    level = jnp.sum(everyone.reshape(8, 2, 4, 2, 2, -1), axis=(2, 4)) / POINTS
    center = jnp.sum(level) / SAMPLES
    spread = jnp.sum((level - center) ** 2) / SAMPLES
    own = lax.dynamic_slice(level, (2 * x, yh, c, 0), (2, 1, 1, level.shape[-1]))
    return (own.reshape(-1) - center) / jnp.sqrt(spread + 1e-06)


def solution(mesh):
    fine = Mesh(mesh.devices.reshape(8, 2, 4, 2, 2), AXES)
    samp = ("yh", "x", "c")
    in_specs = (P(samp, "z"), P(("z",) + samp, "yl"), P("yl"), P("yl"))
    return jax.shard_map(level_correction, mesh=fine, in_specs=in_specs, out_specs=P(samp), check_vma=False)
```
